256 devices in a mesh: tok: 16 (over z, core), vocab: 16 (over y, x).
Axes of the slice: x: 4, y: 4, z: 8, core: 2. Of those that a mesh axis runs over, the one named last changes fastest.
Arguments:
- latent_vectors: float32 [1536, 3584], P('tok'), may hold values from -400 to 400
- unembedding_matrix: float32 [3584, 152064], P(None, ('tok', 'vocab')), may hold values from -0.09375 to 0.09375
- drawn_symbols: int32 [1536], P('tok'), may hold values from 0 to 152063
- piece_extents: int32 [16, 4], P('tok'), may hold values from 1 to 48, 96 in all within a row
- piece_episode_lookup: int32 [16, 4], P('tok'), may hold values from 0 to 1023
- episode_heats: float32 [1024], replicated, may hold values from 0.6 to 1.5
Outputs:
- seg_logprob: float32 [64], P('tok')
The draws below stay inside these ranges and needn't reach their ends.
Inputs may be any that keep to these rules, and one draw needn't show every extreme that they name: `piece_extents`: each row of lengths sums to 96.
All inputs are finite; a program needn't handle non-finite values.
Results may differ from the reference program's by a relative error of at most 0.0003.
Values sent between devices are 32-bit elements; how exact they have to be, the bound alone decides.
A program may use at most 128 MiB of HBM per device.

```python
import math
import jax
import jax.numpy as jnp
import numpy as np
from jax import lax

H = 3584
V = 152064
TOK_DEV = 96
SEG_DEV = 4
EPISODE_NUMBER = 1024
TOKENS = 1536
SEGMENTS = 64
N_TOK = 16
N_VOCAB = 16


def draw_latent_vectors(key, part):
    values = jax.random.normal(key, (TOKENS, H), jnp.float32) * 3.0
    return jnp.clip(values, -400.0, 400.0).astype(jnp.float32)


def place_ends(result, own_key, low, top_value):
    index_at = [jax.random.randint(jax.random.fold_in(own_key, axis), (), 0, length) for axis, length in enumerate(result.shape)]
    widest = result.shape.index(max(result.shape))
    beside = index_at[:widest] + [(index_at[widest] + 1) % result.shape[widest]] + index_at[widest + 1:]
    return result.at[tuple(index_at)].set(low).at[tuple(beside)].set(top_value)


def steps_of(key, dims, shards, least, top_value):
    factor_of, own = 1.0, jax.random.fold_in(key, 6)
    for dim, parts in shards:
        draws = jnp.exp(jax.random.uniform(jax.random.fold_in(own, dim), (parts,), jnp.float32, least / len(shards), top_value / len(shards)))
        factor_of = factor_of * jnp.repeat(draws, dims[dim] // parts).reshape([-1 if axis == dim else 1 for axis in range(len(dims))])
    return factor_of


def ranked_wide(own_key, dims, number_of, lean):
    weights = [min(1 << octave, number_of + 1 - (1 << octave)) * (1 << 20) // math.isqrt((1 << octave) ** lean) + 1 for octave in range((number_of + 1).bit_length()) if 1 << octave <= number_of]
    scale = 1 + sum(weights) // (1 << 30)
    table = np.cumsum(np.array([max(1, weight // scale) for weight in weights]))
    ticket = jax.random.randint(jax.random.fold_in(own_key, 1), dims, 0, int(table[len(weights) - 1]))
    start = jnp.left_shift(1, jnp.searchsorted(jnp.asarray(table, jnp.int32), ticket, side="right").astype(jnp.int32))
    grade = start - 1 + jax.random.randint(jax.random.fold_in(own_key, 4), dims, 0, 1 << 30) % jnp.minimum(start, number_of + 1 - start)
    return jax.random.permutation(jax.random.fold_in(own_key, 2), number_of)[grade].astype(jnp.int32)


def split_up(amount, total, bound, slope):
    weights = [(1 << 20) // math.isqrt(grade ** slope) + 1 for grade in range(2, amount + 1)]
    spare, given = total - bound - (amount - 1), [1] * (amount - 1)
    while spare > 0:
        free = [i for i in range(amount - 1) if given[i] < bound]
        mass, remaining = sum([weights[i] for i in free]), spare
        for i in free:
            addition = min(bound - given[i], max(1, remaining * weights[i] // mass), spare)
            given[i] = given[i] + addition
            spare = spare - addition
    return np.array([bound] + given)


def uneven(rng, count, total, limit, lean):
    if count == 2:
        one = jax.random.randint(rng, (), max(1, total - limit), min(limit, total - 1) + 1)
        return jnp.stack([one, total - one])
    sizes = jnp.asarray(split_up(count, total, limit, lean), jnp.int32)
    twos = (count - 1) // 2
    source_of, sink = sizes[1:1 + 2 * twos:2], sizes[2:2 + 2 * twos:2]
    room = jnp.minimum(source_of - 1, limit - sink)
    moved = jax.random.randint(jax.random.fold_in(rng, 1), (twos,), 0, 1 << 20) % (room + 1)
    sizes = sizes.at[1:1 + 2 * twos:2].set(source_of - moved).at[2:2 + 2 * twos:2].set(sink + moved)
    return sizes[jax.random.permutation(jax.random.fold_in(rng, 2), count)]


def centred(own_key, extent, scale, reach, cuts=(), held_as=jnp.bfloat16):
    result = jax.random.normal(own_key, extent, jnp.float32) * scale
    if len(cuts) > 0:
        result = steps_of(own_key, extent, cuts, -0.22, 0.18) * result
    return jnp.clip(result, min=-reach, max=reach).astype(held_as)


def setup_inputs(seed: int = 0) -> dict:
    seeds = jax.random.split(jax.random.key(seed), 7)
    return {
        "latent_vectors": draw_latent_vectors(jax.random.fold_in(seeds[6], 71), 0),
        "unembedding_matrix": centred(seeds[1], (H, V), H ** -0.5, 0.09375, ((1, 256),), jnp.float32),
        "drawn_symbols": place_ends(ranked_wide(seeds[2], (TOKENS,), V, 2), jax.random.fold_in(seeds[2], 3), 0, V - 1).astype(jnp.int32),
        "piece_extents": jax.vmap(lambda own: uneven(own, SEG_DEV, TOK_DEV, TOK_DEV // 2, 2))(jax.random.split(seeds[3], N_TOK)).reshape((N_TOK, SEG_DEV)).astype(jnp.int32),
        "piece_episode_lookup": place_ends(jax.random.randint(seeds[4], (N_TOK, SEG_DEV), 0, EPISODE_NUMBER), jax.random.fold_in(seeds[4], 1), 0, EPISODE_NUMBER - 1).astype(jnp.int32),
        "episode_heats": jnp.clip(jnp.exp(jax.random.uniform(seeds[5], (EPISODE_NUMBER,), jnp.float32, math.log(0.6), math.log(1.5))), 0.6, 1.5),
    }


def line_heat_divisor(piece_extents, piece_episode_lookup, episode_heats):
    ends = jnp.cumsum(piece_extents, axis=1)
    starts = ends - piece_extents
    position = jnp.arange(TOK_DEV, dtype=jnp.int32)
    piece_episode = ((position[None, None, :] >= starts[:, :, None]) & (position[None, None, :] < ends[:, :, None])).astype(jnp.float32)
    chosen_symbol = (piece_episode_lookup[:, :, None] == jnp.arange(EPISODE_NUMBER, dtype=jnp.int32)[None, None, :]).astype(jnp.float32)
    piece_reciprocal_heat = jnp.einsum("rto,o->rt", chosen_symbol, 1.0 / episode_heats, precision=lax.Precision.HIGHEST)
    symbol_reciprocal_heat = jnp.einsum("sgp,sg->sp", piece_episode, piece_reciprocal_heat, precision=lax.Precision.HIGHEST)
    return piece_episode, symbol_reciprocal_heat.reshape(TOKENS)


def reference(latent_vectors, unembedding_matrix, drawn_symbols, piece_extents, piece_episode_lookup, episode_heats):
    piece_episode, symbol_reciprocal_heat = line_heat_divisor(piece_extents, piece_episode_lookup, episode_heats)
    width = V // (N_TOK * N_VOCAB)

    def block_step(carry, index):
        start = (index * width).astype(jnp.int32)
        columns = lax.dynamic_slice_in_dim(unembedding_matrix, start, width, 1)
        logits = jnp.dot(latent_vectors, columns, preferred_element_type=jnp.float32, precision=lax.Precision.HIGHEST) * symbol_reciprocal_heat[:, None]
        block_top = jnp.max(logits, axis=1)
        block_total = jnp.sum(jnp.exp(logits - block_top[:, None]), axis=1)
        ids = start + jnp.arange(width, dtype=jnp.int32)
        block_picked = jnp.sum(jnp.where(drawn_symbols[:, None] == ids[None, :], logits, 0.0), axis=1)
        return carry, (block_top, block_total, block_picked)

    unused, (tops, totals, pickeds) = lax.scan(block_step, jnp.zeros((), jnp.float32), jnp.arange(N_TOK * N_VOCAB, dtype=jnp.int32))
    top = jnp.max(tops, axis=0)
    total = jnp.sum(totals * jnp.exp(tops - top[None, :]), axis=0)
    picked = jnp.sum(pickeds, axis=0)
    logprob = picked - top - jnp.log(total)
    sums = jnp.einsum("sgp,sp->sg", piece_episode, logprob.reshape(N_TOK, TOK_DEV), precision=lax.Precision.HIGHEST)
    return (sums / piece_extents.astype(jnp.float32)).reshape(SEGMENTS)
```

```python
import functools

import jax
import jax.numpy as jnp
from jax import lax
from jax.experimental import pallas as pl
from jax.experimental.pallas import tpu as pltpu
from jax.sharding import PartitionSpec as P

MESH = pl.DeviceIdType.MESH

NZ = 8
RING = 4
CH = 8
PIECE = 32
UNIT = 128
UNITS = 12
SLOTS = 14
STEPS = 19
NEG = -3.0e38


def kernel(
    x_hbm, w_hbm, sym_ref, ext_ref, look_ref, heat_ref,
    out_ref,
    X, Wf, Wh, Wl, X2, L, META, MT, MS, RB1, A2, RB2,
    own_sem, w_sem, send_sem, recv_sem, msend, mrecv, s1send, r1, s2send, r2,
):
    div, rem = lax.div, lax.rem
    t = lax.axis_index("tok")
    v = lax.axis_index("vocab")
    z, c = div(t, 2), rem(t, 2)
    y, x = div(v, 4), rem(v, 4)
    a = (1 - c) * x + c * y
    width = w_hbm.shape[1]
    sib = (2 * z + (1 - c), v)

    def along_z(step):
        return (2 * rem(z + step + NZ, NZ) + c, v)

    def along_ring(step):
        to = rem(a + step + RING, RING)
        return (t, (1 - c) * (4 * y + to) + c * (4 * to + x))

    def piece(d, sidx, core, j):
        far = div(d, 4)
        return (1 - far) * (6 + 12 * (d - 1) + 4 * j + 2 * sidx + core) + far * (42 + 2 * j + core)

    def mtile(d, sidx, core):
        far = div(d, 4)
        return (1 - far) * (2 + 4 * (d - 1) + 2 * sidx + core) + far * (14 + core)

    def rows(p, q):
        return X.at[pl.ds(pl.multiple_of(p * PIECE + q * CH, CH), CH), :]

    def send(p_from, p_to, q, device):
        pltpu.make_async_remote_copy(
            src_ref=rows(p_from, q), dst_ref=rows(p_to, q),
            send_sem=send_sem, recv_sem=recv_sem.at[p_to * RING + q],
            device_id=device, device_id_type=MESH,
        ).start()

    def arrived(p, q):
        pltpu.make_async_copy(rows(p, q), rows(p, q), recv_sem.at[p * RING + q]).wait()

    def msg(src, dst, ssem, rsem, device):
        pltpu.make_async_remote_copy(
            src_ref=src, dst_ref=dst, send_sem=ssem, recv_sem=rsem,
            device_id=device, device_id_type=MESH,
        ).start()

    def send_meta(i_from, i_to, device):
        msg(META.at[i_from], META.at[i_to], msend, mrecv.at[i_to], device)

    def meta_arrived(i):
        pltpu.make_async_copy(META.at[i], META.at[i], mrecv.at[i]).wait()

    own = [
        pltpu.make_async_copy(
            x_hbm.at[pl.ds(PIECE * j, PIECE), :],
            X.at[pl.ds(pl.multiple_of((2 * j + c) * PIECE, CH), PIECE), :],
            own_sem.at[j],
        )
        for j in range(3)
    ]
    for copy in own:
        copy.start()
    w_copy = pltpu.make_async_copy(w_hbm, Wf, w_sem)
    w_copy.start()

    barrier = pltpu.get_barrier_semaphore()
    for i in range(1, 16):
        pl.semaphore_signal(barrier, inc=1, device_id=(rem(t + i, 16), v), device_id_type=MESH)
        pl.semaphore_signal(barrier, inc=1, device_id=(t, rem(v + i, 16)), device_id_type=MESH)

    lane = lax.broadcasted_iota(jnp.int32, (1, 128), 1)
    scale_row = jnp.zeros((1, 128), jnp.float32)
    start = 0
    for s in range(4):
        end = start + ext_ref[0, s]
        inv = 1.0 / jnp.full((1, 128), heat_ref[look_ref[0, s]], jnp.float32)
        scale_row = jnp.where((lane >= start) & (lane < end), inv, scale_row)
        start = end
    META[c] = jnp.zeros((8, 128), jnp.float32)
    META[c, 0:1, :] = scale_row
    META[c, 1:2, 0:96] = sym_ref[...].astype(jnp.float32)
    MS[...] = jnp.zeros(MS.shape, jnp.float32)
    MT[...] = jnp.zeros(MT.shape, jnp.float32)

    for copy in own:
        copy.wait()
    pl.semaphore_wait(barrier, 30)

    for k in range(4):
        j = min(k, 2)
        q = rem(a + 2 * (k // 3), RING)
        for sidx, s in enumerate((1, -1)):
            send(2 * j + c, piece(1, sidx, c, j), q, along_z(s))
        if k == 0:
            for sidx, s in enumerate((1, -1)):
                send_meta(c, mtile(1, sidx, c), along_z(s))
            send_meta(c, c, sib)
    for j in range(3):
        for q in range(RING):
            send(2 * j + c, 2 * j + c, q, sib)

    w_copy.wait()
    kblk = 128

    def split_w(i, carry):
        ks = pl.ds(pl.multiple_of(i * kblk, kblk), kblk)
        zero = jnp.zeros((kblk, 128), jnp.bfloat16)
        Wh[ks, 512:640] = zero
        Wl[ks, 512:640] = zero
        for lo, hi in ((0, 256), (256, 512), (512, width)):
            w = Wf[ks, lo:hi]
            high = w.astype(jnp.bfloat16)
            Wh[ks, lo:hi] = high
            Wl[ks, lo:hi] = (w - high.astype(jnp.float32)).astype(jnp.bfloat16)
        return carry

    lax.fori_loop(0, w_hbm.shape[0] // kblk, split_w, 0)
    meta_arrived(1 - c)

    column_start = ((t * 16 + v) * width).astype(jnp.float32)
    depth = X.shape[1]

    def unit(u):
        for i in (0, 2):
            for q in range(RING):
                arrived(4 * u + i + (1 - c), q)
        lanes = lax.broadcasted_iota(jnp.int32, (8, 128), 1)
        tile = jnp.zeros((8, 128), jnp.float32)
        for i in range(4):
            p = 4 * u + i
            near = 1 - jnp.minimum(div(p, 6), 1)
            far = div(p, 42)
            mid = 1 - near - far
            pm = p - 6
            idx = near * (i % 2) + far * (14 + i % 2) + mid * (2 + div(pm, 12) * 4 + rem(pm, 4))
            j = near * div(p, 2) + far * div(p - 42, 2) + mid * div(rem(pm, 12), 4)
            turned = pltpu.roll(META[idx], rem(PIECE * (i - j) + 128, 128), 1)
            tile = jnp.where(div(lanes, PIECE) == i, turned, tile)
        MT[0:8, :] = tile
        columns = MT[...].T
        scale = columns[:, 0:1]
        target = columns[:, 1:2] - column_start

        us = pl.multiple_of(u * UNIT, UNIT)
        for k0 in range(0, depth, 512):
            xs = X[pl.ds(us, UNIT), k0 : k0 + 512]
            high = xs.astype(jnp.bfloat16)
            X2[0:UNIT, k0 : k0 + 512] = high
            X2[UNIT : 2 * UNIT, k0 : k0 + 512] = (xs - high.astype(jnp.float32)).astype(jnp.bfloat16)
        for lo, hi in ((0, 256), (256, 512), (512, 640)):
            both = jnp.dot(X2[...], Wh[:, lo:hi], preferred_element_type=jnp.float32)
            low = jnp.dot(X2[0:UNIT, :], Wl[:, lo:hi], preferred_element_type=jnp.float32)
            L[:, lo:hi] = (both[0:UNIT] + (both[UNIT : 2 * UNIT] + low)) * scale
        col = lax.broadcasted_iota(jnp.int32, (UNIT, 640), 1)
        logits = jnp.where(col < width, L[...], NEG)
        top = jnp.max(logits, axis=1, keepdims=True)
        total = jnp.sum(jnp.exp(logits - top), axis=1, keepdims=True)
        picked = jnp.sum(jnp.where(col.astype(jnp.float32) == target, L[...], 0.0), axis=1, keepdims=True)
        lse = top + jnp.log(total)
        col = lax.broadcasted_iota(jnp.int32, (UNIT, 128), 1)
        flat = jnp.where(col == 0, lse, jnp.where(col == 1, picked, 0.0)).T
        lse_row, picked_row = flat[0:1, :], flat[1:2, :]

        def note(k, row):
            MS[k, pl.ds(row, 1), :] = lse_row
            MS[k, pl.ds(row + 3, 1), :] = picked_row

        @pl.when((u >= 1) & (u <= 9))
        def _():
            note(2 * div(u - 1, 3), rem(u - 1, 3))

        @pl.when((u >= 2) & (u <= 10))
        def _():
            note(2 * div(u - 2, 3) + 1, rem(u - 2, 3))

        @pl.when(u >= 10)
        def _():
            note(6, u - 10)

        @pl.when(u <= 1)
        def _():
            note(7, u)

        def report(d, sidx, s):
            for core in range(2):
                msg(
                    MS.at[2 * (d - 1) + sidx], RB1.at[4 * (d - 1) + 2 * sidx + c],
                    s1send, r1.at[4 * (d - 1) + 2 * sidx + c],
                    (2 * rem(z - s * d + NZ, NZ) + core, v),
                )

        @pl.when(u == 1)
        def _():
            msg(MS.at[7], RB1.at[14], s1send, r1.at[14], sib)

        @pl.when((u >= 3) & (u <= 9) & (rem(u, 3) == 0))
        def _():
            report(div(u, 3), 0, 1)

        @pl.when((u >= 4) & (u <= 10) & (rem(u, 3) == 1))
        def _():
            report(div(u, 3), 1, -1)

    def slot(m, sidx):
        late = div(m, 12)
        k = (1 - late) * rem(m, 4) + late * (2 * (m - 12) + sidx)
        return 1 + div(m, 4), k

    def step(n, carry):
        @pl.when((n >= 2) & (n < SLOTS + 2))
        def _():
            m = n - 2
            for sidx in range(2):
                d, k = slot(m, sidx)

                @pl.when(k < 3)
                def _():
                    p = piece(d, sidx, c, k)
                    for gi, g in enumerate((1, -1)):
                        q = rem(a - g + RING, RING)
                        arrived(p, q)

                        @pl.when(k == gi)
                        def _():
                            send(p, p, q, along_ring(g))

                        send(p, p, q, sib)

        @pl.when(n < SLOTS)
        def _():
            for sidx, s in enumerate((1, -1)):
                d, k = slot(n, sidx)
                extra = div(k, 3)
                j = k - extra
                q = rem(a + 2 * extra, RING)
                p = piece(d, sidx, c, j)
                arrived(p, q)

                @pl.when((d < 3) | ((d == 3) & (rem(k, 2) == sidx)))
                def _():
                    send(p, piece(d + 1, sidx, c, j), q, along_z(s))

                @pl.when(k < 3)
                def _():
                    send(p, p, q, along_ring(1))
                    send(p, p, q, along_ring(-1))

                send(p, p, q, sib)

                @pl.when((rem(n, 4) == 0) & (d < 5 - sidx))
                def _():
                    i = mtile(d, sidx, c)
                    meta_arrived(i)

                    @pl.when(d < 4 - sidx)
                    def _():
                        send_meta(i, mtile(d + 1, sidx, c), along_z(s))

                    send_meta(i, i, sib)

        @pl.when((n >= 1) & (n < SLOTS) & (rem(n + 3, 4) == 0))
        def _():
            d = 1 + div(n - 1, 4)
            meta_arrived(mtile(d, 0, 1 - c))

            @pl.when(d < 4)
            def _():
                meta_arrived(mtile(d, 1, 1 - c))

        @pl.when((n >= 4) & (n < SLOTS + 4))
        def _():
            m = n - 4
            for sidx in range(2):
                d, k = slot(m, sidx)

                @pl.when(k < 2)
                def _():
                    p = piece(d, sidx, c, k)
                    q = rem(a + 2, RING)
                    arrived(p, q)
                    send(p, p, q, sib)

        r = n - 5

        @pl.when((n == 4) | ((n >= 5) & (rem(r + 4, 4) < 3)))
        def _():
            first = div(n, 5)
            late = jnp.minimum(first, 1)
            unit(late * (1 + div(r, 4) * 3 + rem(r, 4)))

        return carry

    lax.fori_loop(0, STEPS, step, 0)

    for core in range(2):
        msg(MS.at[6], RB1.at[12 + c], s1send, r1.at[12 + c], (2 * rem(z + 4, NZ) + core, v))
    pltpu.make_async_copy(X.at[pl.ds(0, 180 * CH), :], X.at[pl.ds(0, 180 * CH), :], send_sem).wait()
    pltpu.make_async_copy(META.at[pl.ds(0, 15)], META.at[pl.ds(0, 15)], msend).wait()

    def lse_of(values):
        peak = functools.reduce(jnp.maximum, values)
        return peak + jnp.log(sum(jnp.exp(value - peak) for value in values))

    subl = lax.broadcasted_iota(jnp.int32, (8, 128), 0)

    def merged(tiles):
        return jnp.where(subl < 3, lse_of(tiles), sum(tiles))

    def r1_arrived(i):
        pltpu.make_async_copy(RB1.at[i], RB1.at[i], r1.at[i]).wait()

    for i in range(12):
        r1_arrived(i)
    r1_arrived(14)
    up = pltpu.roll(merged([RB1[4 * k + i] for k in range(3) for i in (0, 1)]), 64, 1)
    down = merged([RB1[4 * k + i] for k in range(3) for i in (2, 3)])
    here = merged([RB1[14], MS[7]])
    hr = pltpu.roll(here, 64, 1)
    near = jnp.where(rem(subl, 3) == 0, here, jnp.where(rem(subl, 3) == 1, pltpu.roll(hr, 1, 0), pltpu.roll(here, 1, 0)))
    first = merged([up, down, near])
    for i in range(12, 14):
        r1_arrived(i)
    there = merged([RB1[12], RB1[13]])
    tr = pltpu.roll(there, 64, 1)
    away = jnp.where(rem(subl, 3) == 0, tr, jnp.where(rem(subl, 3) == 1, there, pltpu.roll(tr, 1, 0)))
    A2[...] = merged([first, away])

    for i in range(1, 16):
        msg(A2, RB2.at[i - 1], s2send, r2.at[i - 1], (t, rem(v + i, 16)))
    pltpu.make_async_copy(RB1.at[pl.ds(0, 15)], RB1.at[pl.ds(0, 15)], s1send).wait()
    for i in range(15):
        pltpu.make_async_copy(RB2.at[i], RB2.at[i], r2.at[i]).wait()
    final = merged([A2[...]] + [RB2[i] for i in range(15)])
    logprob = pltpu.roll(final, 5, 0) - final
    lanes = lax.broadcasted_iota(jnp.int32, (8, 128), 1)
    inside = (div(lanes, PIECE) == c) & (subl < 3)
    position = subl * PIECE + rem(lanes, PIECE)
    result = jnp.zeros((8, 128), jnp.float32)
    start = 0
    for s in range(4):
        size = ext_ref[0, s]
        mask = inside & (position >= start) & (position < start + size)
        value = jnp.sum(jnp.where(mask, logprob, 0.0)) / size.astype(jnp.float32)
        result = jnp.where(lanes == s, value, result)
        start = start + size
    out_ref[...] = result
    pltpu.make_async_copy(RB2, RB2, s2send).wait()


def on_device(latent_vectors, unembedding_matrix, drawn_symbols, piece_extents, piece_episode_lookup, episode_heats):
    rows, depth = latent_vectors.shape
    width = unembedding_matrix.shape[1]
    f32, bf16 = jnp.float32, jnp.bfloat16
    dma, vmem, smem = pltpu.SemaphoreType.DMA, pltpu.VMEM, pltpu.SMEM
    out = pl.pallas_call(
        kernel,
        out_shape=jax.ShapeDtypeStruct((8, 128), f32),
        in_specs=[
            pl.BlockSpec(memory_space=pl.ANY),
            pl.BlockSpec(memory_space=pl.ANY),
            pl.BlockSpec(memory_space=vmem),
            pl.BlockSpec(memory_space=smem),
            pl.BlockSpec(memory_space=smem),
            pl.BlockSpec(memory_space=smem),
        ],
        out_specs=pl.BlockSpec(memory_space=vmem),
        scratch_shapes=[
            vmem((16 * rows, depth), f32),
            vmem((depth, width), f32),
            vmem((depth, 640), bf16),
            vmem((depth, 640), bf16),
            vmem((2 * UNIT, depth), bf16),
            vmem((UNIT, 640), f32),
            vmem((16, 8, 128), f32),
            vmem((128, 128), f32),
            vmem((8, 8, 128), f32),
            vmem((15, 8, 128), f32),
            vmem((8, 128), f32),
            vmem((15, 8, 128), f32),
            dma((3,)), dma, dma, dma((192,)), dma, dma((16,)), dma, dma((15,)), dma, dma((15,)),
        ],
        compiler_params=pltpu.CompilerParams(
            collective_id=0, has_side_effects=True, vmem_limit_bytes=60 * 1024 * 1024
        ),
    )(
        latent_vectors, unembedding_matrix, drawn_symbols.reshape(1, rows),
        piece_extents, piece_episode_lookup, episode_heats,
    )
    return out[0, :4]


def solution(mesh):
    return jax.shard_map(
        on_device,
        mesh=mesh,
        in_specs=(P("tok", None), P(None, ("tok", "vocab")), P("tok"), P("tok", None), P("tok", None), P()),
        out_specs=P("tok"),
        check_vma=False,
    )
```

```python
import functools

import jax
import jax.numpy as jnp
from jax import lax
from jax.experimental import pallas as pl
from jax.experimental.pallas import tpu as pltpu
from jax.sharding import PartitionSpec as P

MESH = pl.DeviceIdType.MESH

NZ = 8
RING = 4
CH = 8
PIECE = 32
UNIT = 128
UNITS = 12
SLOTS = 14
STEPS = 19
NEG = -3.0e38
F8 = jnp.float8_e4m3fn
X_UP, W_UP = 2.0**8, 2.0**12
W_EARLY = 20


def kernel(
    x_hbm, wt_hbm, sym_hbm, ext_hbm, look_hbm, heat_hbm,
    out_ref,
    sym_ref, ext_ref, look_ref, heat_ref, X, Wf, Wh, W8, X2, X8, L, META, MT, MS, RB1, A2, RB2,
    own_sem, small_sem, w_sem, send_sem, recv_sem, msend, mrecv, s1send, r1, s2send, r2,
):
    div, rem = lax.div, lax.rem
    t = lax.axis_index("tok")
    v = lax.axis_index("vocab")
    z, c = div(t, 2), rem(t, 2)
    y, x = div(v, 4), rem(v, 4)
    a = (1 - c) * x + c * y
    width, depth = wt_hbm.shape
    sib = (2 * z + (1 - c), v)

    z_dev = {s: (2 * rem(z + s + NZ, NZ) + c, v) for s in (1, -1)}
    turn = [rem(a + s, RING) for s in range(RING)]
    ring_dev = {s: (t, (1 - c) * (4 * y + turn[s % RING]) + c * (4 * turn[s % RING] + x)) for s in (1, -1, 2)}

    def own_piece(core, j):
        return 2 * j + core if j < 2 else 40 + core

    def piece(d, sidx, core, j):
        far = div(d, 4)
        return (1 - far) * (4 + 12 * (d - 1) + 4 * j + 2 * sidx + core) + far * (44 + 2 * j - 6 * div(j, 2) + core)

    def mtile(d, sidx, core):
        far = div(d, 4)
        return (1 - far) * (2 + 4 * (d - 1) + 2 * sidx + core) + far * (14 + core)

    def rows(p, q):
        return X.at[pl.ds(pl.multiple_of(p * PIECE + q * CH, CH), CH), :]

    def send(p_from, p_to, q, device):
        pltpu.make_async_remote_copy(
            src_ref=rows(p_from, q), dst_ref=rows(p_to, q),
            send_sem=send_sem, recv_sem=recv_sem.at[p_to * RING + q],
            device_id=device, device_id_type=MESH,
        ).start()

    def arrived(p, q):
        pltpu.make_async_copy(rows(p, q), rows(p, q), recv_sem.at[p * RING + q]).wait()

    def msg(src, dst, ssem, rsem, device):
        pltpu.make_async_remote_copy(
            src_ref=src, dst_ref=dst, send_sem=ssem, recv_sem=rsem,
            device_id=device, device_id_type=MESH,
        ).start()

    def send_meta(i_from, i_to, device):
        msg(META.at[i_from], META.at[i_to], msend, mrecv.at[i_to], device)

    def meta_arrived(i):
        pltpu.make_async_copy(META.at[i], META.at[i], mrecv.at[i]).wait()

    barrier = pltpu.get_barrier_semaphore()
    for i in range(1, 16):
        pl.semaphore_signal(barrier, inc=1, device_id=(rem(t + i, 16), v), device_id_type=MESH)
        pl.semaphore_signal(barrier, inc=1, device_id=(t, rem(v + i, 16)), device_id_type=MESH)
    own = [
        pltpu.make_async_copy(
            x_hbm.at[pl.ds(PIECE * j, PIECE), :],
            X.at[pl.ds(pl.multiple_of(own_piece(c, j) * PIECE, CH), PIECE), :],
            own_sem.at[j],
        )
        for j in range(3)
    ]
    small = [
        pltpu.make_async_copy(src, dst, small_sem.at[k])
        for k, (src, dst) in enumerate(
            ((sym_hbm, sym_ref), (ext_hbm, ext_ref), (look_hbm, look_ref), (heat_hbm, heat_ref))
        )
    ]
    w_copy = pltpu.make_async_copy(wt_hbm, Wf, w_sem)
    for copy in own + small + [w_copy]:
        copy.start()
    for copy in small:
        copy.wait()
    lane = lax.broadcasted_iota(jnp.int32, (1, 128), 1)
    scale_row = jnp.zeros((1, 128), jnp.float32)
    start = 0
    for s in range(4):
        end = start + ext_ref[0, s]
        inv = 1.0 / jnp.full((1, 128), heat_ref[look_ref[0, s]], jnp.float32)
        scale_row = jnp.where((lane >= start) & (lane < end), inv, scale_row)
        start = end
    META[c] = jnp.zeros((8, 128), jnp.float32)
    META[c, 0:1, :] = scale_row
    META[c, 1:2, 0:96] = sym_ref[...].astype(jnp.float32)
    MS[...] = jnp.zeros(MS.shape, jnp.float32)
    MT[...] = jnp.zeros(MT.shape, jnp.float32)
    for copy in own:
        copy.wait()
    pl.semaphore_wait(barrier, 30)

    for sidx, s in enumerate((1, -1)):
        send_meta(c, mtile(1, sidx, c), z_dev[s])
    send_meta(c, c, sib)
    for k in range(4):
        j = min(k, 2)
        q = turn[2 * (k // 3)]
        for sidx, s in enumerate((1, -1)):
            send(own_piece(c, j), piece(1, sidx, c, j), q, z_dev[s])
    for j in range(3):
        for q in range(RING):
            send(own_piece(c, j), own_piece(c, j), q, sib)

    w_copy.wait()

    twice = 640 - width

    def split_w(i, carry):
        ks = pl.ds(pl.multiple_of(i * 128, 128), 128)
        kt = pl.ds(pl.multiple_of(depth + i * 128, 128), 128)
        for b in range(5):
            w = Wf[min(128 * b, width - 128) : min(128 * b + 128, width), ks].T
            at = slice(128 * b, 128 * b + 128)
            high = w.astype(jnp.bfloat16)
            Wh[ks, at] = high
            W8[ks, at] = (w * W_UP).astype(F8)
            W8[kt, at] = ((w - high.astype(jnp.float32)) * (W_UP * X_UP)).astype(F8)
        return carry

    lax.fori_loop(0, W_EARLY, split_w, 0)
    meta_arrived(1 - c)

    column_start = ((t * 16 + v) * width).astype(jnp.float32)

    def unit(u):
        for i in (0, 2):
            for q in range(RING):
                arrived(4 * u + i + (1 - c), q)
        lanes = lax.broadcasted_iota(jnp.int32, (8, 128), 1)
        tile = jnp.zeros((8, 128), jnp.float32)
        first, last = 1 - jnp.minimum(u, 1), div(u, 11)
        ten = div(u, 10) - last
        mid = 1 - first - last - ten
        for i in range(4):
            idx = first * (i % 2) + mid * (2 + 4 * div(u - 1, 3) + i) + ten * (i if i < 2 else 12 + i) + last * (14 + i % 2)
            j = (first + last) * (i // 2) + mid * rem(u + 2, 3) + ten * 2
            turned = pltpu.roll(META[idx], rem(PIECE * (i - j) + 128, 128), 1)
            tile = jnp.where(div(lanes, PIECE) == i, turned, tile)
        MT[0:8, :] = tile
        columns = MT[...].T
        scale = columns[:, 0:1]
        target = columns[:, 1:2] - column_start

        us = pl.multiple_of(u * UNIT, UNIT)
        for k0 in range(0, depth, 512):
            xs = X[pl.ds(us, UNIT), k0 : k0 + 512]
            high = xs.astype(jnp.bfloat16)
            X2[:, k0 : k0 + 512] = high
            X8[:, k0 : k0 + 512] = ((xs - high.astype(jnp.float32)) * X_UP).astype(F8)
            X8[:, depth + k0 : depth + k0 + 512] = xs.astype(F8)
        for lo, hi in ((0, 256), (256, 512), (512, 640)):
            main = jnp.dot(X2[...], Wh[:, lo:hi], preferred_element_type=jnp.float32)
            rest = jnp.dot(X8[...], W8[:, lo:hi], preferred_element_type=jnp.float32)
            L[:, lo:hi] = (main + rest * (1.0 / (W_UP * X_UP))) * scale
        col = lax.broadcasted_iota(jnp.int32, (1, 640), 1)
        col = jnp.where(col < 512, col, jnp.where(col < 512 + twice, -(1 << 24), col - twice))
        logits = jnp.where(col >= 0, L[...], NEG)
        top = jnp.max(logits, axis=1, keepdims=True)
        total = jnp.sum(jnp.exp(logits - top), axis=1, keepdims=True)
        picked = jnp.sum(jnp.where(col.astype(jnp.float32) == target, logits, 0.0), axis=1, keepdims=True)
        lse = top + jnp.log(total)
        col = lax.broadcasted_iota(jnp.int32, (UNIT, 128), 1)
        flat = jnp.where(col == 0, lse, jnp.where(col == 1, picked, 0.0)).T
        lse_row, picked_row = flat[0:1, :], flat[1:2, :]

        def note(k, row):
            MS[k, pl.ds(row, 1), :] = lse_row
            MS[k, pl.ds(row + 3, 1), :] = picked_row

        @pl.when((u >= 1) & (u <= 9))
        def _():
            note(div(u - 1, 3), rem(u + 2, 3))

        @pl.when(u >= 10)
        def _():
            note(3, 11 - u)

        @pl.when((u == 0) | (u == 10))
        def _():
            note(4, div(u, 10))

        @pl.when(u == 10)
        def _():
            msg(MS.at[4], RB1.at[14], s1send, r1.at[14], sib)

        @pl.when((u >= 1) & (u <= 9) & (rem(u, 3) == 2))
        def _():
            d = 1 + div(u - 1, 3)
            for sidx, s in enumerate((1, -1)):
                for core in range(2):
                    i = 4 * (d - 1) + 2 * sidx + c
                    msg(MS.at[d - 1], RB1.at[i], s1send, r1.at[i], (2 * rem(z - s * d + NZ, NZ) + core, v))

    def slot(m, sidx):
        late = div(m, 12)
        k = (1 - late) * rem(m, 4) + late * (2 * (m - 12) + sidx)
        return 1 + div(m, 4), k

    def step(n, carry):
        @pl.when(n < SLOTS)
        def _():
            for sidx, s in enumerate((1, -1)):
                d, k = slot(n, sidx)
                extra = div(k, 3)
                j = k - extra
                q = (1 - extra) * a + extra * turn[2]
                p = piece(d, sidx, c, j)
                arrived(p, q)

                @pl.when((d < 3) | ((d == 3) & (rem(k, 2) == sidx)))
                def _():
                    send(p, piece(d + 1, sidx, c, j), q, z_dev[s])

                @pl.when(k < 3)
                def _():
                    send(p, p, q, ring_dev[1])
                    send(p, p, q, ring_dev[-1])

                @pl.when((k < 2) & (d == 4))
                def _():
                    send(p, p, q, ring_dev[2])

                send(p, p, q, sib)

                @pl.when((rem(n, 4) == 0) & (d < 5 - sidx))
                def _():
                    i = mtile(d, sidx, c)
                    meta_arrived(i)

                    @pl.when(d < 4 - sidx)
                    def _():
                        send_meta(i, mtile(d + 1, sidx, c), z_dev[s])

                    send_meta(i, i, sib)

        @pl.when((n >= 2) & (n < SLOTS + 3) & (n != 14))
        def _():
            m = n - 2 - div(n, 15)
            for sidx in range(2):
                d, k = slot(m, sidx)

                @pl.when(k < 3)
                def _():
                    p = piece(d, sidx, c, k)
                    for gi, g in enumerate((1, -1)):
                        q = turn[-g % RING]
                        arrived(p, q)

                        @pl.when((k == gi) & (d < 4))
                        def _():
                            send(p, p, q, ring_dev[g])

                        send(p, p, q, sib)

        @pl.when((n >= 1) & (n < SLOTS) & (rem(n + 3, 4) == 0))
        def _():
            d = 1 + div(n - 1, 4)
            meta_arrived(mtile(d, 0, 1 - c))

            @pl.when(d < 4)
            def _():
                meta_arrived(mtile(d, 1, 1 - c))

        @pl.when((n >= 5) & (n < SLOTS + 5))
        def _():
            m = n - 5
            for sidx in range(2):
                d, k = slot(m, sidx)

                @pl.when(k < 2)
                def _():
                    p = piece(d, sidx, c, k)
                    q = turn[2]
                    arrived(p, q)
                    send(p, p, q, sib)

        @pl.when(n == 0)
        def _():
            lax.fori_loop(W_EARLY, depth // 128, split_w, 0)

        r = n - 5

        @pl.when((n == 0) | ((n >= 5) & (rem(r + 4, 4) < 3)))
        def _():
            some, late = jnp.minimum(n, 1), div(n, 17)
            unit(some * ((1 - late) * (1 + 3 * div(r, 4) + rem(rem(r + 4, 4) + 2, 3)) + late * (n - 7)))

        return carry

    lax.fori_loop(0, STEPS, step, 0)

    for core in range(2):
        msg(MS.at[3], RB1.at[12 + c], s1send, r1.at[12 + c], (2 * rem(z + 4, NZ) + core, v))
    pltpu.make_async_copy(X.at[pl.ds(0, 180 * CH), :], X.at[pl.ds(0, 180 * CH), :], send_sem).wait()
    pltpu.make_async_copy(META.at[pl.ds(0, 15)], META.at[pl.ds(0, 15)], msend).wait()

    def lse_of(values):
        peak = functools.reduce(jnp.maximum, values)
        return peak + jnp.log(sum(jnp.exp(value - peak) for value in values))

    subl = lax.broadcasted_iota(jnp.int32, (8, 128), 0)

    def merged(tiles):
        return jnp.where(subl < 3, lse_of(tiles), sum(tiles))

    def r1_arrived(i):
        pltpu.make_async_copy(RB1.at[i], RB1.at[i], r1.at[i]).wait()

    for i in range(12):
        r1_arrived(i)
    r1_arrived(14)
    up = merged([RB1[4 * k + i] for k in range(3) for i in (0, 1)])
    down = pltpu.roll(merged([RB1[4 * k + i] for k in range(3) for i in (2, 3)]), 64, 1)
    here = merged([RB1[14], MS[4]])
    hr = pltpu.roll(here, 64, 1)
    near = jnp.where(rem(subl, 3) == 0, here, jnp.where(rem(subl, 3) == 1, pltpu.roll(hr, 1, 0), pltpu.roll(here, 1, 0)))
    first = merged([up, down, near])
    for i in range(12, 14):
        r1_arrived(i)
    there = merged([RB1[12], RB1[13]])
    tr = pltpu.roll(there, 64, 1)
    away = jnp.where(rem(subl, 3) == 0, there, pltpu.roll(tr, 1, 0))
    A2[...] = merged([first, away])

    for i in range(1, 16):
        msg(A2, RB2.at[i - 1], s2send, r2.at[i - 1], (t, rem(v + i, 16)))
    pltpu.make_async_copy(RB1.at[pl.ds(0, 15)], RB1.at[pl.ds(0, 15)], s1send).wait()
    for i in range(15):
        pltpu.make_async_copy(RB2.at[i], RB2.at[i], r2.at[i]).wait()
    final = merged([A2[...]] + [RB2[i] for i in range(15)])
    logprob = pltpu.roll(final, 5, 0) - final
    lanes = lax.broadcasted_iota(jnp.int32, (8, 128), 1)
    inside = (div(lanes, PIECE) == c) & (subl < 3)
    position = subl * PIECE + rem(lanes, PIECE)
    result = jnp.zeros((8, 128), jnp.float32)
    start = 0
    for s in range(4):
        size = ext_ref[0, s]
        mask = inside & (position >= start) & (position < start + size)
        value = jnp.sum(jnp.where(mask, logprob, 0.0)) / size.astype(jnp.float32)
        result = jnp.where(lanes == s, value, result)
        start = start + size
    out_ref[...] = result
    pltpu.make_async_copy(RB2, RB2, s2send).wait()


def on_device(latent_vectors, unembedding_matrix, drawn_symbols, piece_extents, piece_episode_lookup, episode_heats):
    rows, depth = latent_vectors.shape
    width = unembedding_matrix.shape[1]
    f32, bf16 = jnp.float32, jnp.bfloat16
    dma, vmem, smem = pltpu.SemaphoreType.DMA, pltpu.VMEM, pltpu.SMEM
    out = pl.pallas_call(
        kernel,
        out_shape=jax.ShapeDtypeStruct((8, 128), f32),
        in_specs=[pl.BlockSpec(memory_space=pl.ANY)] * 6,
        out_specs=pl.BlockSpec(memory_space=vmem),
        scratch_shapes=[
            vmem((1, rows), jnp.int32),
            smem(piece_extents.shape, jnp.int32),
            smem(piece_episode_lookup.shape, jnp.int32),
            smem(episode_heats.shape, f32),
            vmem((16 * rows, depth), f32),
            vmem((width, depth), f32),
            vmem((depth, 640), bf16),
            vmem((2 * depth, 640), F8),
            vmem((UNIT, depth), bf16),
            vmem((UNIT, 2 * depth), F8),
            vmem((UNIT, 640), f32),
            vmem((16, 8, 128), f32),
            vmem((128, 128), f32),
            vmem((8, 8, 128), f32),
            vmem((15, 8, 128), f32),
            vmem((8, 128), f32),
            vmem((15, 8, 128), f32),
            dma((3,)), dma((4,)), dma, dma, dma((192,)), dma, dma((16,)), dma, dma((15,)), dma, dma((15,)),
        ],
        compiler_params=pltpu.CompilerParams(
            collective_id=0, has_side_effects=True, vmem_limit_bytes=60 * 1024 * 1024
        ),
    )(
        latent_vectors, unembedding_matrix.T, drawn_symbols.reshape(1, rows),
        piece_extents, piece_episode_lookup, episode_heats,
    )
    return out[0, :4]


def solution(mesh):
    return jax.shard_map(
        on_device,
        mesh=mesh,
        in_specs=(P("tok", None), P(None, ("tok", "vocab")), P("tok"), P("tok", None), P("tok", None), P()),
        out_specs=P("tok"),
        check_vma=False,
    )
```

```python
import functools

import jax
import jax.numpy as jnp
from jax import lax
from jax.experimental import pallas as pl
from jax.experimental.pallas import tpu as pltpu
from jax.sharding import PartitionSpec as P

MESH = pl.DeviceIdType.MESH

NZ = 8
RING = 4
CH = 8
PIECE = 32
UNIT = 128
UNITS = 12
SLOTS = 14
STEPS = 18
NEG = -3.0e38
F8 = jnp.float8_e4m3fn
X_UP, W_UP = 2.0**8, 2.0**12
W_EARLY, W_STEP = 16, 6


def kernel(
    x_hbm, wt_hbm, sym_hbm, ext_hbm, look_hbm, heat_hbm,
    out_ref,
    sym_ref, ext_ref, look_ref, heat_ref, X, Wf, Wh, W8, X2, X8, L, META, MT, MS, RB1, A2, RB2,
    own_sem, small_sem, w_sem, send_sem, recv_sem, msend, mrecv, s1send, r1, s2send, r2,
):
    div, rem = lax.div, lax.rem
    t = lax.axis_index("tok")
    v = lax.axis_index("vocab")
    z, c = div(t, 2), rem(t, 2)
    y, x = div(v, 4), rem(v, 4)
    a = (1 - c) * x + c * y
    width, depth = wt_hbm.shape
    sib = (2 * z + (1 - c), v)

    z_dev = {s: (2 * rem(z + s + NZ, NZ) + c, v) for s in (1, -1)}
    turn = [rem(a + s, RING) for s in range(RING)]
    ring_dev = {s: (t, (1 - c) * (4 * y + turn[s % RING]) + c * (4 * turn[s % RING] + x)) for s in (1, -1, 2)}

    def own_piece(core, j):
        return 2 * j + core if j < 2 else 40 + core

    def piece(d, sidx, core, j):
        far = div(d, 4)
        return (1 - far) * (4 + 12 * (d - 1) + 4 * j + 2 * sidx + core) + far * (44 + 2 * j - 6 * div(j, 2) + core)

    def mtile(d, sidx, core):
        far = div(d, 4)
        return (1 - far) * (2 + 4 * (d - 1) + 2 * sidx + core) + far * (14 + core)

    def rows(p, q):
        return X.at[pl.ds(pl.multiple_of(p * PIECE + q * CH, CH), CH), :]

    def send(p_from, p_to, q, device):
        pltpu.make_async_remote_copy(
            src_ref=rows(p_from, q), dst_ref=rows(p_to, q),
            send_sem=send_sem, recv_sem=recv_sem.at[p_to * RING + q],
            device_id=device, device_id_type=MESH,
        ).start()

    def arrived(p, q):
        pltpu.make_async_copy(rows(p, q), rows(p, q), recv_sem.at[p * RING + q]).wait()

    def msg(src, dst, ssem, rsem, device):
        pltpu.make_async_remote_copy(
            src_ref=src, dst_ref=dst, send_sem=ssem, recv_sem=rsem,
            device_id=device, device_id_type=MESH,
        ).start()

    def send_meta(i_from, i_to, device):
        msg(META.at[i_from], META.at[i_to], msend, mrecv.at[i_to], device)

    def meta_arrived(i):
        pltpu.make_async_copy(META.at[i], META.at[i], mrecv.at[i]).wait()

    barrier = pltpu.get_barrier_semaphore()
    for i in range(1, 16):
        pl.semaphore_signal(barrier, inc=1, device_id=(rem(t + i, 16), v), device_id_type=MESH)
        pl.semaphore_signal(barrier, inc=1, device_id=(t, rem(v + i, 16)), device_id_type=MESH)
    own = [
        pltpu.make_async_copy(
            x_hbm.at[pl.ds(PIECE * j, PIECE), :],
            X.at[pl.ds(pl.multiple_of(own_piece(c, j) * PIECE, CH), PIECE), :],
            own_sem.at[j],
        )
        for j in range(3)
    ]
    small = [
        pltpu.make_async_copy(src, dst, small_sem.at[k])
        for k, (src, dst) in enumerate(
            ((sym_hbm, sym_ref), (ext_hbm, ext_ref), (look_hbm, look_ref), (heat_hbm, heat_ref))
        )
    ]
    w_copy = pltpu.make_async_copy(wt_hbm, Wf, w_sem)
    for copy in own + small + [w_copy]:
        copy.start()
    for copy in small:
        copy.wait()
    lane = lax.broadcasted_iota(jnp.int32, (1, 128), 1)
    scale_row = jnp.zeros((1, 128), jnp.float32)
    start = 0
    for s in range(4):
        end = start + ext_ref[0, s]
        inv = 1.0 / jnp.full((1, 128), heat_ref[look_ref[0, s]], jnp.float32)
        scale_row = jnp.where((lane >= start) & (lane < end), inv, scale_row)
        start = end
    META[c] = jnp.zeros((8, 128), jnp.float32)
    META[c, 0:1, :] = scale_row
    META[c, 1:2, 0:96] = sym_ref[...].astype(jnp.float32)
    MS[...] = jnp.zeros(MS.shape, jnp.float32)
    MT[...] = jnp.zeros(MT.shape, jnp.float32)
    for copy in own:
        copy.wait()
    pl.semaphore_wait(barrier, 30)

    for sidx, s in enumerate((1, -1)):
        send_meta(c, mtile(1, sidx, c), z_dev[s])
    send_meta(c, c, sib)
    for k in range(4):
        j = min(k, 2)
        q = turn[2 * (k // 3)]
        for sidx, s in enumerate((1, -1)):
            send(own_piece(c, j), piece(1, sidx, c, j), q, z_dev[s])
    for j in range(3):
        for q in range(RING):
            send(own_piece(c, j), own_piece(c, j), q, sib)

    w_copy.wait()

    twice = 640 - width

    def split_w(i, carry):
        ks = pl.ds(pl.multiple_of(i * 128, 128), 128)
        kt = pl.ds(pl.multiple_of(depth + i * 128, 128), 128)
        for b in range(5):
            w = Wf[min(128 * b, width - 128) : min(128 * b + 128, width), ks].T
            at = slice(128 * b, 128 * b + 128)
            high = w.astype(jnp.bfloat16)
            Wh[ks, at] = high
            W8[ks, at] = (w * W_UP).astype(F8)
            W8[kt, at] = ((w - high.astype(jnp.float32)) * (W_UP * X_UP)).astype(F8)
        return carry

    lax.fori_loop(0, W_EARLY, split_w, 0)
    meta_arrived(1 - c)

    column_start = ((t * 16 + v) * width).astype(jnp.float32)

    def unit(u):
        for i in (0, 2):
            for q in range(RING):
                arrived(4 * u + i + (1 - c), q)
        lanes = lax.broadcasted_iota(jnp.int32, (8, 128), 1)
        tile = jnp.zeros((8, 128), jnp.float32)
        first, last = 1 - jnp.minimum(u, 1), div(u, 11)
        ten = div(u, 10) - last
        mid = 1 - first - last - ten
        for i in range(4):
            idx = first * (i % 2) + mid * (2 + 4 * div(u - 1, 3) + i) + ten * (i if i < 2 else 12 + i) + last * (14 + i % 2)
            j = (first + last) * (i // 2) + mid * rem(u + 2, 3) + ten * 2
            turned = pltpu.roll(META[idx], rem(PIECE * (i - j) + 128, 128), 1)
            tile = jnp.where(div(lanes, PIECE) == i, turned, tile)
        MT[0:8, :] = tile
        columns = MT[...].T
        scale = columns[:, 0:1]
        target = columns[:, 1:2] - column_start

        us = pl.multiple_of(u * UNIT, UNIT)
        for k0 in range(0, depth, 512):
            xs = X[pl.ds(us, UNIT), k0 : k0 + 512]
            high = xs.astype(jnp.bfloat16)
            X2[:, k0 : k0 + 512] = high
            X8[:, k0 : k0 + 512] = ((xs - high.astype(jnp.float32)) * X_UP).astype(F8)
            X8[:, depth + k0 : depth + k0 + 512] = xs.astype(F8)
        for lo, hi in ((0, 256), (256, 512), (512, 640)):
            main = jnp.dot(X2[...], Wh[:, lo:hi], preferred_element_type=jnp.float32)
            rest = jnp.dot(X8[...], W8[:, lo:hi], preferred_element_type=jnp.float32)
            L[:, lo:hi] = (main + rest * (1.0 / (W_UP * X_UP))) * scale
        col = lax.broadcasted_iota(jnp.int32, (1, 640), 1)
        col = jnp.where(col < 512, col, jnp.where(col < 512 + twice, -(1 << 24), col - twice))
        logits = jnp.where(col >= 0, L[...], NEG)
        top = jnp.max(logits, axis=1, keepdims=True)
        total = jnp.sum(jnp.exp(logits - top), axis=1, keepdims=True)
        picked = jnp.sum(jnp.where(col.astype(jnp.float32) == target, logits, 0.0), axis=1, keepdims=True)
        lse = top + jnp.log(total)
        col = lax.broadcasted_iota(jnp.int32, (UNIT, 128), 1)
        flat = jnp.where(col == 0, lse, jnp.where(col == 1, picked, 0.0)).T
        lse_row, picked_row = flat[0:1, :], flat[1:2, :]

        def note(k, row):
            MS[k, pl.ds(row, 1), :] = lse_row
            MS[k, pl.ds(row + 3, 1), :] = picked_row

        @pl.when((u >= 1) & (u <= 9))
        def _():
            note(div(u - 1, 3), rem(u + 2, 3))

        @pl.when(u >= 10)
        def _():
            note(3, 11 - u)

        @pl.when((u == 0) | (u == 10))
        def _():
            note(4, div(u, 10))

        @pl.when(u == 10)
        def _():
            msg(MS.at[4], RB1.at[14], s1send, r1.at[14], sib)

        @pl.when((u >= 1) & (u <= 9) & (rem(u, 3) == 2))
        def _():
            d = 1 + div(u - 1, 3)
            for sidx, s in enumerate((1, -1)):
                for core in range(2):
                    i = 4 * (d - 1) + 2 * sidx + c
                    msg(MS.at[d - 1], RB1.at[i], s1send, r1.at[i], (2 * rem(z - s * d + NZ, NZ) + core, v))

    def slot(m, sidx):
        late = div(m, 12)
        k = (1 - late) * rem(m, 4) + late * (2 * (m - 12) + sidx)
        return 1 + div(m, 4), k

    def step(n, carry):
        @pl.when(n < SLOTS)
        def _():
            for sidx, s in enumerate((1, -1)):
                d, k = slot(n, sidx)
                extra = div(k, 3)
                j = k - extra
                q = (1 - extra) * a + extra * turn[2]
                p = piece(d, sidx, c, j)
                arrived(p, q)

                @pl.when((d < 3) | ((d == 3) & (rem(k, 2) == sidx)))
                def _():
                    send(p, piece(d + 1, sidx, c, j), q, z_dev[s])

                @pl.when(k < 3)
                def _():
                    send(p, p, q, ring_dev[1])
                    send(p, p, q, ring_dev[-1])

                @pl.when((k < 2) & (d == 4))
                def _():
                    send(p, p, q, ring_dev[2])

                send(p, p, q, sib)

                @pl.when((rem(n, 4) == 0) & (d < 5 - sidx))
                def _():
                    i = mtile(d, sidx, c)
                    meta_arrived(i)

                    @pl.when(d < 4 - sidx)
                    def _():
                        send_meta(i, mtile(d + 1, sidx, c), z_dev[s])

                    send_meta(i, i, sib)

        @pl.when((n >= 2) & (n < SLOTS + 3) & (n != 14))
        def _():
            m = n - 2 - div(n, 15)
            for sidx in range(2):
                d, k = slot(m, sidx)

                @pl.when(k < 3)
                def _():
                    p = piece(d, sidx, c, k)
                    for gi, g in enumerate((1, -1)):
                        q = turn[-g % RING]
                        arrived(p, q)

                        @pl.when((k == gi) & (d < 4))
                        def _():
                            send(p, p, q, ring_dev[g])

                        send(p, p, q, sib)

        @pl.when((n >= 1) & (n < SLOTS) & (rem(n + 3, 4) == 0))
        def _():
            d = 1 + div(n - 1, 4)
            meta_arrived(mtile(d, 0, 1 - c))

            @pl.when(d < 4)
            def _():
                meta_arrived(mtile(d, 1, 1 - c))

        @pl.when((n >= 6) & (n < 16))
        def _():
            m = n - 6 + div(n, 13) + 2 * div(n, 15)
            for sidx in range(2):
                d, k = slot(m, sidx)

                @pl.when(k < 2)
                def _():
                    p = piece(d, sidx, c, k)
                    q = turn[2]
                    arrived(p, q)
                    send(p, p, q, sib)

        @pl.when(n < 2)
        def _():
            at = W_EARLY + n * W_STEP
            lax.fori_loop(at, at + W_STEP, split_w, 0)

        r = n - 5
        quarter = rem(r + 4, 4)

        @pl.when((n == 2) | ((n >= 5) & (quarter != 1)) | (n >= 14))
        def _():
            some, late, end = jnp.minimum(div(n, 3), 1), div(n, 14), div(n, 16)
            usual = 1 + 3 * div(r, 4) + rem(quarter + 2, 4)
            unit(some * ((1 - late) * usual + (late - end) * (n - 7) + end * (27 - n)))

        return carry

    lax.fori_loop(0, STEPS, step, 0)

    for core in range(2):
        msg(MS.at[3], RB1.at[12 + c], s1send, r1.at[12 + c], (2 * rem(z + 4, NZ) + core, v))
    pltpu.make_async_copy(X.at[pl.ds(0, 180 * CH), :], X.at[pl.ds(0, 180 * CH), :], send_sem).wait()
    pltpu.make_async_copy(META.at[pl.ds(0, 15)], META.at[pl.ds(0, 15)], msend).wait()

    def lse_of(values):
        peak = functools.reduce(jnp.maximum, values)
        return peak + jnp.log(sum(jnp.exp(value - peak) for value in values))

    subl = lax.broadcasted_iota(jnp.int32, (8, 128), 0)

    def merged(tiles):
        return jnp.where(subl < 3, lse_of(tiles), sum(tiles))

    def r1_arrived(i):
        pltpu.make_async_copy(RB1.at[i], RB1.at[i], r1.at[i]).wait()

    for i in range(12):
        r1_arrived(i)
    r1_arrived(14)
    up = merged([RB1[4 * k + i] for k in range(3) for i in (0, 1)])
    down = pltpu.roll(merged([RB1[4 * k + i] for k in range(3) for i in (2, 3)]), 64, 1)
    here = merged([RB1[14], MS[4]])
    hr = pltpu.roll(here, 64, 1)
    near = jnp.where(rem(subl, 3) == 0, here, jnp.where(rem(subl, 3) == 1, pltpu.roll(hr, 1, 0), pltpu.roll(here, 1, 0)))
    first = merged([up, down, near])
    for i in range(12, 14):
        r1_arrived(i)
    there = merged([RB1[12], RB1[13]])
    tr = pltpu.roll(there, 64, 1)
    away = jnp.where(rem(subl, 3) == 0, there, pltpu.roll(tr, 1, 0))
    A2[...] = merged([first, away])

    for i in range(1, 16):
        msg(A2, RB2.at[i - 1], s2send, r2.at[i - 1], (t, rem(v + i, 16)))
    pltpu.make_async_copy(RB1.at[pl.ds(0, 15)], RB1.at[pl.ds(0, 15)], s1send).wait()
    for i in range(15):
        pltpu.make_async_copy(RB2.at[i], RB2.at[i], r2.at[i]).wait()
    final = merged([A2[...]] + [RB2[i] for i in range(15)])
    logprob = pltpu.roll(final, 5, 0) - final
    lanes = lax.broadcasted_iota(jnp.int32, (8, 128), 1)
    inside = (div(lanes, PIECE) == c) & (subl < 3)
    position = subl * PIECE + rem(lanes, PIECE)
    start = 0
    for s in range(4):
        size = ext_ref[0, s]
        mask = inside & (position >= start) & (position < start + size)
        out_ref[s] = jnp.sum(jnp.where(mask, logprob, 0.0)) / size.astype(jnp.float32)
        start = start + size
    pltpu.make_async_copy(RB2, RB2, s2send).wait()


def on_device(latent_vectors, unembedding_matrix, drawn_symbols, piece_extents, piece_episode_lookup, episode_heats):
    rows, depth = latent_vectors.shape
    width = unembedding_matrix.shape[1]
    f32, bf16 = jnp.float32, jnp.bfloat16
    dma, vmem, smem = pltpu.SemaphoreType.DMA, pltpu.VMEM, pltpu.SMEM
    out = pl.pallas_call(
        kernel,
        out_shape=jax.ShapeDtypeStruct((4,), f32),
        in_specs=[pl.BlockSpec(memory_space=pl.ANY)] * 6,
        out_specs=pl.BlockSpec(memory_space=smem),
        scratch_shapes=[
            vmem((1, rows), jnp.int32),
            smem(piece_extents.shape, jnp.int32),
            smem(piece_episode_lookup.shape, jnp.int32),
            smem(episode_heats.shape, f32),
            vmem((16 * rows, depth), f32),
            vmem((width, depth), f32),
            vmem((depth, 640), bf16),
            vmem((2 * depth, 640), F8),
            vmem((UNIT, depth), bf16),
            vmem((UNIT, 2 * depth), F8),
            vmem((UNIT, 640), f32),
            vmem((16, 8, 128), f32),
            vmem((128, 128), f32),
            vmem((8, 8, 128), f32),
            vmem((15, 8, 128), f32),
            vmem((8, 128), f32),
            vmem((15, 8, 128), f32),
            dma((3,)), dma((4,)), dma, dma, dma((192,)), dma, dma((16,)), dma, dma((15,)), dma, dma((15,)),
        ],
        compiler_params=pltpu.CompilerParams(
            collective_id=0, has_side_effects=True, vmem_limit_bytes=60 * 1024 * 1024
        ),
    )(
        latent_vectors, unembedding_matrix.T, drawn_symbols.reshape(1, rows),
        piece_extents, piece_episode_lookup, episode_heats,
    )
    return out


def solution(mesh):
    return jax.shard_map(
        on_device,
        mesh=mesh,
        in_specs=(P("tok", None), P(None, ("tok", "vocab")), P("tok"), P("tok", None), P("tok", None), P()),
        out_specs=P("tok"),
        check_vma=False,
    )
```

```python
import functools

import jax
import jax.numpy as jnp
from jax import lax
from jax.experimental import pallas as pl
from jax.experimental.pallas import tpu as pltpu
from jax.sharding import PartitionSpec as P

MESH = pl.DeviceIdType.MESH

NZ = 8
RING = 4
CH = 8
PIECE = 32
UNIT = 128
UNITS = 12
SLOTS = 14
STEPS = 18
NEG = -3.0e38
F8 = jnp.float8_e4m3fn
X_UP, W_UP = 2.0**8, 2.0**12
W_EARLY, W_STEP = 16, 6


def kernel(
    x_hbm, wt_hbm, sym_hbm, ext_hbm, look_hbm, heat_hbm,
    out_ref,
    sym_ref, ext_ref, look_ref, heat_ref, X, Wf, Wh, W8, X2, X8, L, META, MT, MS, RB1, A2, RB2,
    own_sem, small_sem, w_sem, send_sem, recv_sem, msend, mrecv, s1send, r1, s2send, r2,
):
    div, rem = lax.div, lax.rem
    t = lax.axis_index("tok")
    v = lax.axis_index("vocab")
    z, c = div(t, 2), rem(t, 2)
    y, x = div(v, 4), rem(v, 4)
    a = (1 - c) * x + c * y
    width, depth = wt_hbm.shape
    sib = (2 * z + (1 - c), v)

    z_dev = {s: (2 * rem(z + s + NZ, NZ) + c, v) for s in (1, -1)}
    turn = [rem(a + s, RING) for s in range(RING)]
    ring_dev = {s: (t, (1 - c) * (4 * y + turn[s % RING]) + c * (4 * turn[s % RING] + x)) for s in (1, -1, 2)}

    def own_piece(core, j):
        return 2 * j + core if j < 2 else 40 + core

    def piece(d, sidx, core, j):
        far = div(d, 4)
        return (1 - far) * (4 + 12 * (d - 1) + 4 * j + 2 * sidx + core) + far * (44 + 2 * j - 6 * div(j, 2) + core)

    def mtile(d, sidx, core):
        far = div(d, 4)
        return (1 - far) * (2 + 4 * (d - 1) + 2 * sidx + core) + far * (14 + core)

    def rows(p, q):
        return X.at[pl.ds(pl.multiple_of(p * PIECE + q * CH, CH), CH), :]

    def send(p_from, p_to, q, device):
        pltpu.make_async_remote_copy(
            src_ref=rows(p_from, q), dst_ref=rows(p_to, q),
            send_sem=send_sem, recv_sem=recv_sem.at[p_to * RING + q],
            device_id=device, device_id_type=MESH,
        ).start()

    def arrived(p, q):
        pltpu.make_async_copy(rows(p, q), rows(p, q), recv_sem.at[p * RING + q]).wait()

    def msg(src, dst, ssem, rsem, device):
        pltpu.make_async_remote_copy(
            src_ref=src, dst_ref=dst, send_sem=ssem, recv_sem=rsem,
            device_id=device, device_id_type=MESH,
        ).start()

    def send_meta(i_from, i_to, device):
        msg(META.at[i_from], META.at[i_to], msend, mrecv.at[i_to], device)

    def meta_arrived(i):
        pltpu.make_async_copy(META.at[i], META.at[i], mrecv.at[i]).wait()

    barrier = pltpu.get_barrier_semaphore()
    for i in range(1, 16):
        pl.semaphore_signal(barrier, inc=1, device_id=(rem(t + i, 16), v), device_id_type=MESH)
        pl.semaphore_signal(barrier, inc=1, device_id=(t, rem(v + i, 16)), device_id_type=MESH)
    own = [
        pltpu.make_async_copy(
            x_hbm.at[pl.ds(PIECE * j, PIECE), :],
            X.at[pl.ds(pl.multiple_of(own_piece(c, j) * PIECE, CH), PIECE), :],
            own_sem.at[j],
        )
        for j in range(3)
    ]
    small = [
        pltpu.make_async_copy(src, dst, small_sem.at[k])
        for k, (src, dst) in enumerate(
            ((sym_hbm, sym_ref), (ext_hbm, ext_ref), (look_hbm, look_ref), (heat_hbm, heat_ref))
        )
    ]
    w_copy = pltpu.make_async_copy(wt_hbm, Wf, w_sem)
    for copy in own + small:
        copy.start()
    for copy in small:
        copy.wait()
    lane = lax.broadcasted_iota(jnp.int32, (1, 128), 1)
    scale_row = jnp.zeros((1, 128), jnp.float32)
    start = 0
    for s in range(4):
        end = start + ext_ref[0, s]
        inv = 1.0 / jnp.full((1, 128), heat_ref[look_ref[0, s]], jnp.float32)
        scale_row = jnp.where((lane >= start) & (lane < end), inv, scale_row)
        start = end
    META[c] = jnp.zeros((8, 128), jnp.float32)
    META[c, 0:1, :] = scale_row
    META[c, 1:2, 0:96] = sym_ref[...].astype(jnp.float32)
    MS[...] = jnp.zeros(MS.shape, jnp.float32)
    MT[...] = jnp.zeros(MT.shape, jnp.float32)
    for copy in own:
        copy.wait()
    w_copy.start()
    pl.semaphore_wait(barrier, 30)

    for sidx, s in enumerate((1, -1)):
        send_meta(c, mtile(1, sidx, c), z_dev[s])
    send_meta(c, c, sib)
    for k in range(4):
        j = min(k, 2)
        q = turn[2 * (k // 3)]
        for sidx, s in enumerate((1, -1)):
            send(own_piece(c, j), piece(1, sidx, c, j), q, z_dev[s])
    for j in range(3):
        for q in range(RING):
            send(own_piece(c, j), own_piece(c, j), q, sib)

    w_copy.wait()

    twice = 640 - width

    def split_w(i, carry):
        ks = pl.ds(pl.multiple_of(i * 128, 128), 128)
        kt = pl.ds(pl.multiple_of(depth + i * 128, 128), 128)
        for b in range(5):
            w = Wf[min(128 * b, width - 128) : min(128 * b + 128, width), ks].T
            at = slice(128 * b, 128 * b + 128)
            high = w.astype(jnp.bfloat16)
            Wh[ks, at] = high
            W8[ks, at] = (w * W_UP).astype(F8)
            W8[kt, at] = ((w - high.astype(jnp.float32)) * (W_UP * X_UP)).astype(F8)
        return carry

    lax.fori_loop(0, W_EARLY, split_w, 0)
    meta_arrived(1 - c)

    column_start = ((t * 16 + v) * width).astype(jnp.float32)

    def unit(u):
        for i in (0, 2):
            for q in range(RING):
                arrived(4 * u + i + (1 - c), q)
        lanes = lax.broadcasted_iota(jnp.int32, (8, 128), 1)
        tile = jnp.zeros((8, 128), jnp.float32)
        first, last = 1 - jnp.minimum(u, 1), div(u, 11)
        ten = div(u, 10) - last
        mid = 1 - first - last - ten
        for i in range(4):
            idx = first * (i % 2) + mid * (2 + 4 * div(u - 1, 3) + i) + ten * (i if i < 2 else 12 + i) + last * (14 + i % 2)
            j = (first + last) * (i // 2) + mid * rem(u + 2, 3) + ten * 2
            turned = pltpu.roll(META[idx], rem(PIECE * (i - j) + 128, 128), 1)
            tile = jnp.where(div(lanes, PIECE) == i, turned, tile)
        MT[0:8, :] = tile
        columns = MT[...].T
        scale = columns[:, 0:1]
        target = columns[:, 1:2] - column_start

        us = pl.multiple_of(u * UNIT, UNIT)
        for k0 in range(0, depth, 512):
            xs = X[pl.ds(us, UNIT), k0 : k0 + 512]
            high = xs.astype(jnp.bfloat16)
            X2[:, k0 : k0 + 512] = high
            X8[:, k0 : k0 + 512] = ((xs - high.astype(jnp.float32)) * X_UP).astype(F8)
            X8[:, depth + k0 : depth + k0 + 512] = xs.astype(F8)
        for lo, hi in ((0, 256), (256, 512), (512, 640)):
            main = jnp.dot(X2[...], Wh[:, lo:hi], preferred_element_type=jnp.float32)
            rest = jnp.dot(X8[...], W8[:, lo:hi], preferred_element_type=jnp.float32)
            L[:, lo:hi] = (main + rest * (1.0 / (W_UP * X_UP))) * scale
        col = lax.broadcasted_iota(jnp.int32, (1, 640), 1)
        col = jnp.where(col < 512, col, jnp.where(col < 512 + twice, -(1 << 24), col - twice))
        logits = jnp.where(col >= 0, L[...], NEG)
        top = jnp.max(logits, axis=1, keepdims=True)
        total = jnp.sum(jnp.exp(logits - top), axis=1, keepdims=True)
        picked = jnp.sum(jnp.where(col.astype(jnp.float32) == target, logits, 0.0), axis=1, keepdims=True)
        lse = top + jnp.log(total)
        col = lax.broadcasted_iota(jnp.int32, (UNIT, 128), 1)
        flat = jnp.where(col == 0, lse, jnp.where(col == 1, picked, 0.0)).T
        lse_row, picked_row = flat[0:1, :], flat[1:2, :]

        def note(k, row):
            MS[k, pl.ds(row, 1), :] = lse_row
            MS[k, pl.ds(row + 3, 1), :] = picked_row

        @pl.when((u >= 1) & (u <= 9))
        def _():
            note(div(u - 1, 3), rem(u + 2, 3))

        @pl.when(u >= 10)
        def _():
            note(3, 11 - u)

        @pl.when((u == 0) | (u == 10))
        def _():
            note(4, div(u, 10))

        @pl.when(u == 10)
        def _():
            msg(MS.at[4], RB1.at[14], s1send, r1.at[14], sib)

        @pl.when((u >= 1) & (u <= 9) & (rem(u, 3) == 2))
        def _():
            d = 1 + div(u - 1, 3)
            for sidx, s in enumerate((1, -1)):
                for core in range(2):
                    i = 4 * (d - 1) + 2 * sidx + c
                    msg(MS.at[d - 1], RB1.at[i], s1send, r1.at[i], (2 * rem(z - s * d + NZ, NZ) + core, v))

    def slot(m, sidx):
        late = div(m, 12)
        k = (1 - late) * rem(m, 4) + late * (2 * (m - 12) + sidx)
        return 1 + div(m, 4), k

    def step(n, carry):
        @pl.when(n < SLOTS)
        def _():
            for sidx, s in enumerate((1, -1)):
                d, k = slot(n, sidx)
                extra = div(k, 3)
                j = k - extra
                q = (1 - extra) * a + extra * turn[2]
                p = piece(d, sidx, c, j)
                arrived(p, q)

                @pl.when((d < 3) | ((d == 3) & (rem(k, 2) == sidx)))
                def _():
                    send(p, piece(d + 1, sidx, c, j), q, z_dev[s])

                @pl.when(k < 3)
                def _():
                    send(p, p, q, ring_dev[1])
                    send(p, p, q, ring_dev[-1])

                @pl.when((k < 2) & (d == 4))
                def _():
                    send(p, p, q, ring_dev[2])

                send(p, p, q, sib)

                @pl.when((rem(n, 4) == 0) & (d < 5 - sidx))
                def _():
                    i = mtile(d, sidx, c)
                    meta_arrived(i)

                    @pl.when(d < 4 - sidx)
                    def _():
                        send_meta(i, mtile(d + 1, sidx, c), z_dev[s])

                    send_meta(i, i, sib)

        @pl.when((n >= 2) & (n < SLOTS + 3) & (n != 14))
        def _():
            m = n - 2 - div(n, 15)
            for sidx in range(2):
                d, k = slot(m, sidx)

                @pl.when(k < 3)
                def _():
                    p = piece(d, sidx, c, k)
                    for gi, g in enumerate((1, -1)):
                        q = turn[-g % RING]
                        arrived(p, q)

                        @pl.when((k == gi) & (d < 4))
                        def _():
                            send(p, p, q, ring_dev[g])

                        send(p, p, q, sib)

        @pl.when((n >= 1) & (n < SLOTS) & (rem(n + 3, 4) == 0))
        def _():
            d = 1 + div(n - 1, 4)
            meta_arrived(mtile(d, 0, 1 - c))

            @pl.when(d < 4)
            def _():
                meta_arrived(mtile(d, 1, 1 - c))

        @pl.when((n >= 6) & (n < 16))
        def _():
            m = n - 6 + div(n, 13) + 2 * div(n, 15)
            for sidx in range(2):
                d, k = slot(m, sidx)

                @pl.when(k < 2)
                def _():
                    p = piece(d, sidx, c, k)
                    q = turn[2]
                    arrived(p, q)
                    send(p, p, q, sib)

        @pl.when(n < 2)
        def _():
            at = W_EARLY + n * W_STEP
            lax.fori_loop(at, at + W_STEP, split_w, 0)

        r = n - 5
        quarter = rem(r + 4, 4)

        @pl.when((n == 2) | ((n >= 5) & (quarter != 1)) | (n >= 14))
        def _():
            some, late, end = jnp.minimum(div(n, 3), 1), div(n, 14), div(n, 16)
            usual = 1 + 3 * div(r, 4) + rem(quarter + 2, 4)
            unit(some * ((1 - late) * usual + (late - end) * (n - 7) + end * (27 - n)))

        return carry

    lax.fori_loop(0, STEPS, step, 0)

    for core in range(2):
        msg(MS.at[3], RB1.at[12 + c], s1send, r1.at[12 + c], (2 * rem(z + 4, NZ) + core, v))
    pltpu.make_async_copy(X.at[pl.ds(0, 180 * CH), :], X.at[pl.ds(0, 180 * CH), :], send_sem).wait()
    pltpu.make_async_copy(META.at[pl.ds(0, 15)], META.at[pl.ds(0, 15)], msend).wait()

    def lse_of(values):
        peak = functools.reduce(jnp.maximum, values)
        return peak + jnp.log(sum(jnp.exp(value - peak) for value in values))

    subl = lax.broadcasted_iota(jnp.int32, (8, 128), 0)

    def merged(tiles):
        return jnp.where(subl < 3, lse_of(tiles), sum(tiles))

    def r1_arrived(i):
        pltpu.make_async_copy(RB1.at[i], RB1.at[i], r1.at[i]).wait()

    for i in range(12):
        r1_arrived(i)
    r1_arrived(14)
    up = merged([RB1[4 * k + i] for k in range(3) for i in (0, 1)])
    down = pltpu.roll(merged([RB1[4 * k + i] for k in range(3) for i in (2, 3)]), 64, 1)
    here = merged([RB1[14], MS[4]])
    hr = pltpu.roll(here, 64, 1)
    near = jnp.where(rem(subl, 3) == 0, here, jnp.where(rem(subl, 3) == 1, pltpu.roll(hr, 1, 0), pltpu.roll(here, 1, 0)))
    first = merged([up, down, near])
    for i in range(12, 14):
        r1_arrived(i)
    there = merged([RB1[12], RB1[13]])
    tr = pltpu.roll(there, 64, 1)
    away = jnp.where(rem(subl, 3) == 0, there, pltpu.roll(tr, 1, 0))
    A2[...] = merged([first, away])

    for i in range(1, 16):
        msg(A2, RB2.at[i - 1], s2send, r2.at[i - 1], (t, rem(v + i, 16)))
    pltpu.make_async_copy(RB1.at[pl.ds(0, 15)], RB1.at[pl.ds(0, 15)], s1send).wait()
    for i in range(15):
        pltpu.make_async_copy(RB2.at[i], RB2.at[i], r2.at[i]).wait()
    final = merged([A2[...]] + [RB2[i] for i in range(15)])
    logprob = pltpu.roll(final, 5, 0) - final
    lanes = lax.broadcasted_iota(jnp.int32, (8, 128), 1)
    inside = (div(lanes, PIECE) == c) & (subl < 3)
    position = subl * PIECE + rem(lanes, PIECE)
    start = 0
    for s in range(4):
        size = ext_ref[0, s]
        mask = inside & (position >= start) & (position < start + size)
        out_ref[s] = jnp.sum(jnp.where(mask, logprob, 0.0)) / size.astype(jnp.float32)
        start = start + size
    pltpu.make_async_copy(RB2, RB2, s2send).wait()


def on_device(latent_vectors, unembedding_matrix, drawn_symbols, piece_extents, piece_episode_lookup, episode_heats):
    rows, depth = latent_vectors.shape
    width = unembedding_matrix.shape[1]
    f32, bf16 = jnp.float32, jnp.bfloat16
    dma, vmem, smem = pltpu.SemaphoreType.DMA, pltpu.VMEM, pltpu.SMEM
    out = pl.pallas_call(
        kernel,
        out_shape=jax.ShapeDtypeStruct((4,), f32),
        in_specs=[pl.BlockSpec(memory_space=pl.ANY)] * 6,
        out_specs=pl.BlockSpec(memory_space=smem),
        scratch_shapes=[
            vmem((1, rows), jnp.int32),
            smem(piece_extents.shape, jnp.int32),
            smem(piece_episode_lookup.shape, jnp.int32),
            smem(episode_heats.shape, f32),
            vmem((16 * rows, depth), f32),
            vmem((width, depth), f32),
            vmem((depth, 640), bf16),
            vmem((2 * depth, 640), F8),
            vmem((UNIT, depth), bf16),
            vmem((UNIT, 2 * depth), F8),
            vmem((UNIT, 640), f32),
            vmem((16, 8, 128), f32),
            vmem((128, 128), f32),
            vmem((8, 8, 128), f32),
            vmem((15, 8, 128), f32),
            vmem((8, 128), f32),
            vmem((15, 8, 128), f32),
            dma((3,)), dma((4,)), dma, dma, dma((192,)), dma, dma((16,)), dma, dma((15,)), dma, dma((15,)),
        ],
        compiler_params=pltpu.CompilerParams(
            collective_id=0, has_side_effects=True, vmem_limit_bytes=60 * 1024 * 1024
        ),
    )(
        latent_vectors, unembedding_matrix.T, drawn_symbols.reshape(1, rows),
        piece_extents, piece_episode_lookup, episode_heats,
    )
    return out


def solution(mesh):
    return jax.shard_map(
        on_device,
        mesh=mesh,
        in_specs=(P("tok", None), P(None, ("tok", "vocab")), P("tok"), P("tok", None), P("tok", None), P()),
        out_specs=P("tok"),
        check_vma=False,
    )
```
